32 devices in a mesh: leaf: 32 (over z, y, x, core).
Axes of the slice: x: 2, y: 2, z: 4, core: 2. Of those that a mesh axis runs over, the one named last changes fastest.
Arguments:
- shots: float32 [32768, 2048], P('leaf'), may hold values from -6 to 6
- leaf_inverse: float32 [32768, 1024], P('leaf'), may hold values from -0.1875 to 0.1875
- leaf_basis: float32 [8192, 1024], P('leaf'), may hold values from -0.1875 to 0.1875
- leaf_back: float32 [32768, 256], P('leaf'), may hold values from -0.375 to 0.375
- level_one: float32 [8192, 1024], P('leaf'), may hold values from -0.25 to 0.25
- level_two: float32 [4096, 1024], P('leaf'), may hold values from -0.25 to 0.25
- level_three: float32 [2048, 1024], P('leaf'), may hold values from -0.25 to 0.25
- top_inverse: float32 [1024, 1024], P('leaf'), may hold values from -0.1 to 0.1, as said below
Outputs:
- solution: float32 [32768, 2048], P('leaf')
The draws below stay inside these ranges and needn't reach their ends.
Inputs may be any that keep to these rules, and one draw needn't show every extreme that they name: top_inverse is symmetric.
All inputs are finite; a program needn't handle non-finite values.
Results may differ from the reference program's by a relative error of at most 0.0001.
Values sent between devices are 32-bit elements; how exact they have to be, the bound alone decides.
A program may use at most 128 MiB of HBM per device.

```python
import math
import jax
import jax.numpy as jnp
from jax import lax

LEAF_ROWS = 1024
LOW_RANK = 256
SHOT_COUNT = 2048
TOP_NODES = 4
N_LEAF = 32


def draw_top_inverse(key, part):
    order = TOP_NODES * LOW_RANK
    entries = jax.random.normal(key, (order, order), jnp.float32)
    symmetric = (entries + entries.T) * (0.5 ** 0.5 / math.sqrt(order))
    return jnp.clip(symmetric, -0.1, 0.1)


def block_scale(key, shape, cuts, smallest, largest):
    level, own = 1.0, jax.random.fold_in(key, 6)
    for axis_at, parts in cuts:
        draws = jnp.exp(jax.random.uniform(jax.random.fold_in(own, axis_at), (parts,), jnp.float32, smallest / len(cuts), largest / len(cuts)))
        level = level * jnp.repeat(draws, shape[axis_at] // parts).reshape([-1 if axis == axis_at else 1 for axis in range(len(shape))])
    return level


def gaussian(rng, extent, scale, bound, split=(), held_as=jnp.bfloat16):
    values = jax.random.normal(rng, extent, jnp.float32) * scale
    if len(split) > 0:
        values = block_scale(rng, extent, split, -0.22, 0.18) * values
    return jnp.clip(values, min=-bound, max=bound).astype(held_as)


def setup_inputs(seed: int = 0) -> dict:
    streams_of = jax.random.split(jax.random.key(seed), 9)
    shots = gaussian(streams_of[0], (N_LEAF * LEAF_ROWS, SHOT_COUNT), 1.0, 6.0, ((0, 32),), jnp.float32)
    leaf_inverse = gaussian(streams_of[1], (N_LEAF * LEAF_ROWS, LEAF_ROWS), LEAF_ROWS ** -0.5, 0.1875, ((0, 32),), jnp.float32)
    leaf_basis = gaussian(streams_of[2], (N_LEAF * LOW_RANK, LEAF_ROWS), LEAF_ROWS ** -0.5, 0.1875, ((0, 32),), jnp.float32)
    leaf_back = gaussian(streams_of[3], (N_LEAF * LEAF_ROWS, LOW_RANK), LOW_RANK ** -0.5, 0.375, ((0, 32),), jnp.float32)
    level_one = gaussian(streams_of[4], (N_LEAF * LOW_RANK, 4 * LOW_RANK), (2 * LOW_RANK) ** -0.5, 0.25, ((0, 32),), jnp.float32)
    level_two = gaussian(streams_of[5], (N_LEAF * LOW_RANK // 2, 4 * LOW_RANK), (2 * LOW_RANK) ** -0.5, 0.25, ((0, 32),), jnp.float32)
    level_three = gaussian(streams_of[6], (N_LEAF * LOW_RANK // 4, 4 * LOW_RANK), (2 * LOW_RANK) ** -0.5, 0.25, ((0, 32),), jnp.float32)
    top_inverse = draw_top_inverse(jax.random.fold_in(streams_of[8], 71), 0)
    return {"shots": shots, "leaf_inverse": leaf_inverse, "leaf_basis": leaf_basis, "leaf_back": leaf_back, "level_one": level_one, "level_two": level_two, "level_three": level_three, "top_inverse": top_inverse}


def reference(shots, leaf_inverse, leaf_basis, leaf_back, level_one, level_two, level_three, top_inverse):
    highest = lax.Precision.HIGHEST
    leaves = N_LEAF
    rhs_blocks = shots.reshape(leaves, LEAF_ROWS, SHOT_COUNT)
    eliminators = leaf_inverse.reshape(leaves, LEAF_ROWS, LEAF_ROWS)
    solved = jnp.einsum("nij,njs->nis", eliminators, rhs_blocks, precision=highest)
    bases = leaf_basis.reshape(leaves, LOW_RANK, LEAF_ROWS)
    reduced = jnp.einsum("nrm,nms->nrs", bases, solved, precision=highest)
    stored = []
    for factors in (level_one, level_two, level_three):
        nodes = reduced.shape[0] // 2
        blocks = factors.reshape(nodes, 2 * LOW_RANK, 4 * LOW_RANK)
        inverse_block = blocks[:, :, :2 * LOW_RANK]
        reduce_block = blocks[:, :, 2 * LOW_RANK:3 * LOW_RANK]
        back_block = blocks[:, :, 3 * LOW_RANK:]
        stacked = reduced.reshape(nodes, 2 * LOW_RANK, SHOT_COUNT)
        coupled = jnp.einsum("nij,njs->nis", inverse_block, stacked, precision=highest)
        reduced = jnp.einsum("nir,nis->nrs", reduce_block, coupled, precision=highest)
        stored.append((coupled, back_block))
    gathered = reduced.reshape(TOP_NODES * LOW_RANK, SHOT_COUNT)
    top_solution = jnp.dot(top_inverse, gathered, precision=highest)
    coefficient = top_solution.reshape(TOP_NODES, LOW_RANK, SHOT_COUNT)
    for coupled, back_block in reversed(stored):
        remainder = coupled - jnp.einsum("nir,nrs->nis", back_block, coefficient, precision=highest)
        coefficient = remainder.reshape(-1, LOW_RANK, SHOT_COUNT)
    backs = leaf_back.reshape(leaves, LEAF_ROWS, LOW_RANK)
    result = solved - jnp.einsum("nmr,nrs->nms", backs, coefficient, precision=highest)
    return result.reshape(leaves * LEAF_ROWS, SHOT_COUNT)
```

```python
import jax
import jax.numpy as jnp
from jax import lax
from jax.sharding import PartitionSpec as P

LEVELS = 3
CHUNKS = 2
HIGH = lax.Precision.HIGH


def partner_2(value, bit):
    return lax.ppermute(value, "leaf", [(i, i ^ 1 << bit) for i in range(lax.axis_size("leaf"))])


def is_upper(bit):
    return lax.axis_index("leaf") >> bit & 1 == 1


def dot(a, b):
    return jnp.dot(a, b, precision=HIGH)


def gather_rows(values, bits):
    rows = values.shape[0]
    position = lax.axis_index("leaf")
    values = values[None]
    done = []
    for bit in bits:
        partner = partner_2(values, bit)
        low = sum(1 for b in done if b < bit)
        done.append(bit)
        lead = values.shape[0]
        upper = is_upper(bit)
        inner = 2**low
        v = values.reshape(lead // inner, 1, inner, rows, -1)
        p = partner.reshape(lead // inner, 1, inner, rows, -1)
        values = jnp.where(upper, jnp.concatenate([p, v], 1), jnp.concatenate([v, p], 1))
        values = values.reshape(2 * lead, rows, -1)
    return values.reshape(values.shape[0] * rows, -1)


def gather_top(values, bits):
    position_total = len(bits)
    for bit in bits:
        partner = partner_2(values, bit)
        values = jnp.where(
            is_upper(bit), jnp.concatenate([partner, values], 0), jnp.concatenate([values, partner], 0)
        )
    return values


def halves(values, bit):
    half = values.shape[1] // 2
    upper = is_upper(bit).astype(jnp.int32)
    mine = lax.dynamic_slice_in_dim(values, upper * half, half, 1)
    other = lax.dynamic_slice_in_dim(values, (1 - upper) * half, half, 1)
    return mine, other


def prepare(factors, bit, rank):
    upper = is_upper(bit)
    k = factors[:, : 2 * rank]
    k = jnp.where(upper, jnp.concatenate([k[:, rank:], k[:, :rank]], 1), k)
    q = factors[:, 2 * rank : 3 * rank]
    g = lax.dot_general(q, k, (((0,), (0,)), ((), ())), precision=HIGH)
    kf = jnp.concatenate([k, -factors[:, 3 * rank :]], 1)
    kf = jnp.where(upper, jnp.concatenate([kf[rank:], kf[:rank]], 0), kf)
    return g, kf


def shards(
    shots, leaf_inverse, leaf_basis, leaf_back, level_one, level_two, level_three, top_inverse
):
    rank = leaf_basis.shape[0]
    size = lax.axis_size("leaf")
    total_bits = size.bit_length() - 1
    f1 = gather_rows(level_one, (0,))
    f2 = gather_rows(level_two, (1, 0))
    f3 = gather_rows(level_three, (1, 2, 0))
    node_inverse = gather_rows(top_inverse, (1, 2, 0))
    ahead = dot(leaf_basis, leaf_inverse)
    prepared = [prepare(f, bit, rank) for bit, f in enumerate((f1, f2, f3))]
    width = shots.shape[1] // CHUNKS
    found = []
    for c in range(CHUNKS):
        reduced = dot(ahead, shots[:, c * width : (c + 1) * width])
        kept = []
        for bit, (g, kf) in enumerate(prepared):
            mine, other = halves(reduced, bit)
            partner = partner_2(other, bit)
            kept.append((mine, partner))
            reduced = dot(g[:, :rank], mine) + dot(g[:, rank:], partner)
        pieces = gather_top(reduced, tuple(range(LEVELS, total_bits)))
        coefficient = dot(node_inverse, pieces)
        for bit in range(LEVELS - 1, -1, -1):
            mine, partner = kept[bit]
            g, kf = prepared[bit]
            stack = jnp.concatenate([mine, partner, coefficient], 0)
            partner_half = partner_2(dot(kf[rank:], stack), bit)
            own_half = dot(kf[:rank], stack)
            coefficient = jnp.where(
                is_upper(bit),
                jnp.concatenate([partner_half, own_half], 1),
                jnp.concatenate([own_half, partner_half], 1),
            )
        found.append(coefficient)
    solved = dot(leaf_inverse, shots)
    return solved - dot(leaf_back, jnp.concatenate(found, 1))


def solution(mesh):
    return jax.shard_map(
        shards,
        mesh=mesh,
        in_specs=(P("leaf", None),) * 8,
        out_specs=P("leaf", None),
        check_vma=False,
    )
```

```python
import jax
import jax.numpy as jnp
from jax import lax
from jax.sharding import PartitionSpec as P

LEVELS = 3
CHUNKS = 1
HIGH = lax.Precision.HIGH


def partner_of(value, mask):
    return lax.ppermute(value, "leaf", [(i, i ^ mask) for i in range(lax.axis_size("leaf"))])


def is_upper(bit):
    return lax.axis_index("leaf") >> bit & 1 == 1


def dot(a, b):
    return jnp.dot(a, b, precision=HIGH)


def swapped(values, axis):
    half = values.shape[axis] // 2
    low = lax.slice_in_dim(values, 0, half, axis=axis)
    high = lax.slice_in_dim(values, half, 2 * half, axis=axis)
    return lax.concatenate([high, low], axis)


def in_order(stack, bits):
    for axis, bit in enumerate(bits):
        if bit is not None:
            stack = jnp.where(is_upper(bit), swapped(stack, axis), stack)
    return stack


def halves(values, bit):
    half = values.shape[1] // 2
    upper = is_upper(bit).astype(jnp.int32)
    mine = lax.dynamic_slice_in_dim(values, upper * half, half, 1)
    other = lax.dynamic_slice_in_dim(values, (1 - upper) * half, half, 1)
    return mine, other


def prepare(factors, bit, rank):
    k = factors[:, : 2 * rank]
    k = jnp.where(is_upper(bit), swapped(k, 1), k)
    q = factors[:, 2 * rank : 3 * rank]
    g = lax.dot_general(q, k, (((0,), (0,)), ((), ())), precision=HIGH)
    return g, k, factors[:, 3 * rank :]


def shards(
    shots, leaf_inverse, leaf_basis, leaf_back, level_one, level_two, level_three, top_inverse
):
    rank, _ = leaf_basis.shape
    total_bits = lax.axis_size("leaf").bit_length() - 1
    width = shots.shape[1] // CHUNKS

    one_partner = partner_of(level_one, 1)
    two = jnp.stack([level_two, partner_of(level_two, 2)])
    cols = level_three.shape[1]
    third_rows = level_three.shape[0]
    late = jnp.concatenate([level_three, top_inverse.reshape(-1, cols)], 0)
    late = jnp.stack([late, partner_of(late, 2)])
    two_partner = partner_of(two, 1)
    late = jnp.stack([late, partner_of(late, 4)])
    late_partner = partner_of(late, 1)

    ahead = dot(leaf_basis, leaf_inverse)
    f1 = jnp.concatenate([level_one, one_partner], 0)
    f2 = in_order(jnp.stack([two, two_partner], 1), (None, 0)).reshape(-1, cols)
    late = jnp.stack([late, late_partner], 2)
    f3 = in_order(late[:, :, :, :third_rows], (None, 1, 0)).reshape(-1, cols)
    inverse = in_order(late[:, :, :, third_rows:], (2, 1, 0))
    inverse = inverse.reshape(rank, -1)
    nodes = 2 ** (total_bits - LEVELS)
    prepared = [prepare(f, bit, rank) for bit, f in enumerate((f1, f2, f3))]

    solved = dot(leaf_inverse, shots)
    chunks = [dot(ahead, shots[:, c * width : (c + 1) * width]) for c in range(CHUNKS)]
    coupled = [[] for _ in chunks]
    for bit, (g, k, f) in enumerate(prepared):
        for c in range(CHUNKS):
            mine, other = halves(chunks[c], bit)
            partner = partner_of(other, 1 << bit)
            coupled[c].append(dot(k[:, :rank], mine) + dot(k[:, rank:], partner))
            chunks[c] = dot(g[:, :rank], mine) + dot(g[:, rank:], partner)
    for c in range(CHUNKS):
        pieces = [chunks[c]]
        for k in range(1, nodes):
            pieces.append(partner_of(chunks[c], k << LEVELS))
        stack = jnp.stack(pieces).reshape((2,) * (total_bits - LEVELS) + chunks[c].shape)
        stack = in_order(stack, range(total_bits - 1, LEVELS - 1, -1))
        chunks[c] = dot(inverse, stack.reshape(nodes * rank, -1))
    for bit in range(LEVELS - 1, -1, -1):
        g, k, f = prepared[bit]
        for c in range(CHUNKS):
            z = coupled[c][bit]
            partner_half = partner_of(z[rank:] - dot(f[rank:], chunks[c]), 1 << bit)
            own_half = z[:rank] - dot(f[:rank], chunks[c])
            chunks[c] = jnp.where(
                is_upper(bit),
                jnp.concatenate([partner_half, own_half], 1),
                jnp.concatenate([own_half, partner_half], 1),
            )
    return solved - dot(leaf_back, jnp.concatenate(chunks, 1))


def solution(mesh):
    return jax.shard_map(
        shards,
        mesh=mesh,
        in_specs=(P("leaf", None),) * 8,
        out_specs=P("leaf", None),
        check_vma=False,
    )
```
